32 devices in a mesh: rows: 8 (over y, x, core), width: 4 (over z).
Axes of the slice: x: 2, y: 2, z: 4, core: 2. Of those that a mesh axis runs over, the one named last changes fastest.
Arguments:
- one_query: float32 [7168, 7168], P('rows', 'width'), may hold values from -0.09375 to 0.09375
- other_query: float32 [7168, 7168], P('rows', 'width'), may hold values from -0.0625 to 0.0625
- one_key: float32 [7168, 1024], P('rows', 'width'), may hold values from -0.09375 to 0.09375
- other_key: float32 [7168, 1024], P('rows', 'width'), may hold values from -0.0625 to 0.0625
- one_value: float32 [7168, 1024], P('rows', 'width'), may hold values from -0.09375 to 0.09375
- other_value: float32 [7168, 1024], P('rows', 'width'), may hold values from -0.0625 to 0.0625
- mix_share: float32 [7168], P('rows'), may hold values from 0.2 to 0.8
- norm_train: float32 [7168], P(('rows', 'width')), may hold values from 0.25 to 1.75
- norm_step: float32 [7168], P(('rows', 'width')), may hold values from -0.3 to 0.3
Outputs:
- final_query: bfloat16 [7168, 7168], P(None, 'width')
- final_key: bfloat16 [7168, 1024], P(None, 'width')
- final_value: bfloat16 [7168, 1024], P(None, 'width')
- column_query: float32 [7168], P('width')
- column_key: float32 [1024], P('width')
- column_value: float32 [1024], P('width')
- serve_norm: bfloat16 [7168], replicated
The draws below stay inside these ranges and needn't reach their ends.
All inputs are finite; a program needn't handle non-finite values.
Results may differ from the reference program's by a relative error of at most 0.001.
Values may be sent and summed in bfloat16 or wider, within the bound.
A program may use at most 128 MiB of HBM per device.

```python
import jax
import jax.numpy as jnp
from jax import lax

D_MODEL = 7168
Q_DIM = 7168
KV_DIM = 1024


def spiked(result, rng, source, target, shards_of, factor):
    owner, partner = [(jnp.arange(result.shape[position]) // (result.shape[position] // shards_of)).reshape([-1 if axis == position else 1 for axis in range(result.ndim)]) for position in (source, target)]
    chosen = jax.random.permutation(rng, shards_of)[partner]
    strong = (owner == chosen) | (owner == (partner + shards_of // 2) % shards_of)
    return jnp.where(strong, factor * result, result)


def block_levels(stream_key, shape, shards, smallest, top_value):
    def one(position, shards_of):
        heights = jax.random.uniform(jax.random.fold_in(jax.random.fold_in(stream_key, 6), position), (shards_of,), jnp.float32, smallest / len(shards), top_value / len(shards))
        return jnp.repeat(jnp.exp(heights), shape[position] // shards_of).reshape((-1,) + (1,) * (len(shape) - position - 1))

    loudness = one(*shards[0])
    for cut in shards[1:]:
        loudness = loudness * one(*cut)
    return loudness


def bell_draw(rng, dims, deviation, most, cuts=(), dtype=jnp.bfloat16):
    entries = jax.random.normal(rng, dims, jnp.float32) * deviation
    if len(cuts) > 0:
        entries = block_levels(rng, dims, cuts, -0.22, 0.18) * entries
    return jnp.clip(entries, min=-most, max=most).astype(dtype)


def heavy_noise(key, extent, scale, most, split, heavy, dtype=jnp.bfloat16):
    values = scale * jax.random.normal(key, extent, jnp.float32)
    if split:
        values = values * block_levels(key, extent, split, -0.22, 0.18)
    return jnp.clip(spiked(values, jax.random.fold_in(key, 3), *heavy), -most, most).astype(dtype)


def setup_inputs(seed: int = 0) -> dict:
    seeds = jax.random.split(jax.random.key(seed), 10)
    return {
        "one_query": heavy_noise(seeds[0], (D_MODEL, Q_DIM), D_MODEL ** -0.5, 0.09375, ((0, 8), (1, 4)), (0, 1, 8, 2.0), jnp.float32),
        "other_query": bell_draw(seeds[1], (D_MODEL, Q_DIM), D_MODEL ** -0.5, 0.0625, ((0, 8), (1, 4)), jnp.float32),
        "one_key": heavy_noise(seeds[2], (D_MODEL, KV_DIM), D_MODEL ** -0.5, 0.09375, ((0, 8), (1, 4)), (0, 1, 8, 2.0), jnp.float32),
        "other_key": bell_draw(seeds[3], (D_MODEL, KV_DIM), D_MODEL ** -0.5, 0.0625, ((0, 8), (1, 4)), jnp.float32),
        "one_value": heavy_noise(seeds[4], (D_MODEL, KV_DIM), D_MODEL ** -0.5, 0.09375, ((0, 8), (1, 4)), (0, 1, 8, 2.0), jnp.float32),
        "other_value": bell_draw(seeds[5], (D_MODEL, KV_DIM), D_MODEL ** -0.5, 0.0625, ((0, 8), (1, 4)), jnp.float32),
        "mix_share": jnp.clip(0.2 + 0.6 * jax.random.uniform(seeds[6], (D_MODEL,), jnp.float32) ** block_levels(seeds[6], (D_MODEL,), ((0, 8),), -0.2, 0.2), 0.2, 0.8),
        "norm_train": jnp.clip(1.0 + 0.15 * jax.random.normal(seeds[7], (D_MODEL,), jnp.float32), 0.25, 1.75),
        "norm_step": jnp.clip(jax.random.uniform(seeds[8], (D_MODEL,), jnp.float32, -0.3, 0.3) * block_levels(seeds[8], (D_MODEL,), ((0, 32),), -0.4, 0.0), -0.3, 0.3),
    }


def reference(one_query, other_query, one_key, other_key, one_value, other_value, mix_share, norm_train, norm_step):
    result_query = mix_share[:, None] * one_query + (1.0 - mix_share[:, None]) * other_query
    result_key = mix_share[:, None] * one_key + (1.0 - mix_share[:, None]) * other_key
    result_value = mix_share[:, None] * one_value + (1.0 - mix_share[:, None]) * other_value
    column_query = jnp.sqrt(lax.optimization_barrier(jnp.sum(result_query * result_query, axis=0)))
    final_query = (result_query / column_query).astype(jnp.bfloat16)
    column_key = jnp.sqrt(lax.optimization_barrier(jnp.sum(result_key * result_key, axis=0)))
    final_key = (result_key / column_key).astype(jnp.bfloat16)
    column_value = jnp.sqrt(lax.optimization_barrier(jnp.sum(result_value * result_value, axis=0)))
    final_value = (result_value / column_value).astype(jnp.bfloat16)
    serve_norm = (norm_train + norm_step).astype(jnp.bfloat16)
    return (final_query, final_key, final_value, column_query, column_key, column_value, serve_norm)
```

```python
import jax
import jax.numpy as jnp
from jax import lax
from jax.experimental import pallas as pl
from jax.experimental.pallas import tpu as pltpu
from jax.sharding import PartitionSpec as P

MESH = pl.DeviceIdType.MESH
LANES = 128


def kernel(
    n_rows,
    n_width,
    share,
    norm_in,
    one_query,
    other_query,
    one_key,
    other_key,
    one_value,
    other_value,
    *refs,
):
    blocks = refs[: 2 + one_query.shape[1] // one_key.shape[1]]
    col_query, col_key, col_value, norm_all, first, second, part, in_sem = refs[len(blocks) :][:8]
    norm_send, norm_recv, slab_send, slab_recv, sum_send, sum_recv = refs[len(blocks) + 8 :][:6]
    ring_send, ring_recv, twin_send, twin_recv = refs[len(blocks) + 14 :]
    me = lax.axis_index("rows")
    lane = lax.axis_index("width")
    depth, wide = one_key.shape
    groups = [
        (one_key, other_key, blocks[0], col_key, 0),
        (one_value, other_value, blocks[1], col_value, 0),
    ] + [
        (one_query, other_query, blocks[2 + j], col_query, j * wide)
        for j in range(one_query.shape[1] // wide)
    ]
    tile = 64 if depth % 64 == 0 else 16
    half = depth // 2

    loads = []
    for g, (one, other, _, _, at) in enumerate(groups):
        a = pltpu.make_async_copy(one.at[:, pl.ds(at, wide)], first.at[g], in_sem.at[0, g])
        b = pltpu.make_async_copy(other.at[:, pl.ds(at, wide)], second.at[g], in_sem.at[1, g])
        a.start()
        b.start()
        loads.append((a, b))

    norm_all[me, lane] = norm_in[...]

    barrier = pltpu.get_barrier_semaphore()
    for d in range(1, n_rows):
        pl.semaphore_signal(
            barrier, inc=1, device_id={"rows": lax.rem(me + d, n_rows)}, device_id_type=MESH
        )
    for d in range(1, n_width):
        pl.semaphore_signal(
            barrier, inc=1, device_id={"width": lax.rem(lane + d, n_width)}, device_id_type=MESH
        )
    pl.semaphore_wait(barrier, n_rows + n_width - 2)

    norm_copies = []
    for d in range(1, n_width):
        copy = pltpu.make_async_remote_copy(
            src_ref=norm_all.at[me, lane],
            dst_ref=norm_all.at[me, lane],
            send_sem=norm_send.at[d],
            recv_sem=norm_recv.at[d],
            device_id={"width": lax.rem(lane + d, n_width)},
            device_id_type=MESH,
        )
        copy.start()
        norm_copies.append(copy)

    for g in range(len(groups)):
        loads[g][0].wait()
        loads[g][1].wait()

        def mix(i, acc):
            rows = pl.ds(pl.multiple_of(i * tile, tile), tile)
            s = share[rows, :]
            s = jnp.concatenate([s] * (wide // LANES), axis=1)
            r = s * first[g, rows, :] + (1.0 - s) * second[g, rows, :]
            first[g, rows, :] = r
            return acc + jnp.sum((r * r).reshape(tile // 8, 8, wide), axis=0)

        acc = lax.fori_loop(0, depth // tile, mix, jnp.zeros((8, wide), jnp.float32))
        part[me, g] = jnp.sum(acc, axis=0, keepdims=True)

    sum_copies = []
    for d in range(1, n_rows):
        copy = pltpu.make_async_remote_copy(
            src_ref=part.at[me],
            dst_ref=part.at[me],
            send_sem=sum_send.at[d],
            recv_sem=sum_recv.at[d],
            device_id={"rows": lax.rem(me + d, n_rows)},
            device_id_type=MESH,
        )
        copy.start()
        sum_copies.append(copy)

    for copy in norm_copies:
        copy.wait_recv()
    slab_copies = []
    for d in range(1, n_rows):
        copy = pltpu.make_async_remote_copy(
            src_ref=norm_all.at[me],
            dst_ref=norm_all.at[me],
            send_sem=slab_send.at[d],
            recv_sem=slab_recv.at[d],
            device_id={"rows": lax.rem(me + d, n_rows)},
            device_id_type=MESH,
        )
        copy.start()
        slab_copies.append(copy)

    for copy in sum_copies:
        copy.wait_recv()

    core = lax.rem(me, 2)
    chip = me // 2
    chips = n_rows // 2
    reach = chips // 2

    def fold(c):
        return jnp.where(c < reach, c, 3 * reach - 1 - c)

    place = fold(chip)

    def device_at(step):
        return fold(lax.rem(place + step + chips, chips)) * 2 + core

    twin = me + 1 - 2 * core
    ahead = (device_at(1), device_at(-1))
    waits = []

    def region(g, owner, way, hop):
        if hop < reach:
            rows = pl.ds(pl.multiple_of(owner * depth, half), depth)
        else:
            rows = pl.ds(pl.multiple_of(owner * depth + way * half, half), half)
        return blocks[g].at[rows, :]

    def ring_copy(g, owner, way, hop):
        ref = region(g, owner, way, hop)
        copy = pltpu.make_async_remote_copy(
            src_ref=ref,
            dst_ref=ref,
            send_sem=ring_send.at[way, hop - 1, g],
            recv_sem=ring_recv.at[way, hop - 1, g],
            device_id={"rows": ahead[way]},
            device_id_type=MESH,
        )
        copy.start()
        return copy

    def twin_copy(g, owner, way, hop, slot):
        ref = region(g, owner, way, hop)
        copy = pltpu.make_async_remote_copy(
            src_ref=ref,
            dst_ref=ref,
            send_sem=twin_send.at[slot, g],
            recv_sem=twin_recv.at[slot, g],
            device_id={"rows": twin},
            device_id_type=MESH,
        )
        copy.start()
        waits.append(copy)

    flying = {}
    for g, (_, _, out, col, at) in enumerate(groups):
        total = part[0, g]
        for p in range(1, n_rows):
            total = total + part[p, g]
        scale = jnp.sqrt(total)
        col[:, pl.ds(at, wide)] = scale
        inverse = 1.0 / scale

        def narrow(i, carry):
            rows = pl.ds(pl.multiple_of(i * tile, tile), tile)
            here = pl.ds(pl.multiple_of(me * depth + i * tile, tile), tile)
            out[here, :] = (first[g, rows, :] * inverse).astype(out.dtype)
            return carry

        lax.fori_loop(0, depth // tile, narrow, 0)
        for way in range(2):
            flying[way, 1, g] = ring_copy(g, me, way, 1)
        twin_copy(g, me, 0, 0, 0)

    for hop in range(1, reach + 1):
        for g in range(len(groups)):
            for way in range(2):
                copy = flying[way, hop, g]
                copy.wait_recv()
                owner = device_at(-hop if way == 0 else hop)
                if hop < reach:
                    flying[way, hop + 1, g] = ring_copy(g, owner, way, hop + 1)
                twin_copy(g, owner, way, hop, 1 + 2 * (hop - 1) + way)

    for copy in flying.values():
        copy.wait_send()
    for copy in waits:
        copy.wait()
    for copy in norm_copies + sum_copies:
        copy.wait_send()
    for copy in slab_copies:
        copy.wait()


def store(*refs):
    outs, sem = refs[-8:-1], refs[-1]
    blocks, small = refs[:-12], refs[-12:-8]
    wide = blocks[0].shape[1]
    pairs = [(blocks[0], outs[1]), (blocks[1], outs[2])] + list(zip(small, outs[3:]))
    for j, block in enumerate(blocks[2:]):
        pairs.append((block, outs[0].at[:, pl.ds(j * wide, wide)]))
    copies = [pltpu.make_async_copy(src, dst, sem.at[i]) for i, (src, dst) in enumerate(pairs)]
    for copy in copies:
        copy.start()
    for copy in copies:
        copy.wait()


def solution(mesh):
    n_rows, n_width = mesh.shape["rows"], mesh.shape["width"]

    def shards(
        one_query,
        other_query,
        one_key,
        other_key,
        one_value,
        other_value,
        mix_share,
        norm_train,
        norm_step,
    ):
        depth, wide = one_key.shape
        wide_query = one_query.shape[1]
        count = 2 + wide_query // wide
        piece = norm_train.shape[0]
        padded = -(-piece // LANES) * LANES
        share = jnp.broadcast_to(mix_share[:, None], (depth, LANES))
        norm = jnp.pad(norm_train + norm_step, (0, padded - piece)).reshape(1, padded)
        total = depth * n_rows
        reach = n_rows // 4
        hbm = pl.BlockSpec(memory_space=pltpu.HBM)
        vmem = pl.BlockSpec(memory_space=pltpu.VMEM)
        dma = pltpu.SemaphoreType.DMA
        out_shape = (pltpu.VMEM((total, wide), jnp.bfloat16),) * count + (
            pltpu.VMEM((1, wide_query), jnp.float32),
            pltpu.VMEM((1, wide), jnp.float32),
            pltpu.VMEM((1, wide), jnp.float32),
            pltpu.VMEM((n_rows, n_width, 1, padded), jnp.float32),
        )
        gathered = pl.pallas_call(
            lambda *refs: kernel(n_rows, n_width, *refs),
            out_shape=out_shape,
            in_specs=[vmem] * 2 + [hbm] * 6,
            out_specs=[vmem] * (count + 4),
            scratch_shapes=[
                pltpu.VMEM((count, depth, wide), jnp.float32),
                pltpu.VMEM((count, depth, wide), jnp.float32),
                pltpu.VMEM((n_rows, count, 1, wide), jnp.float32),
                dma((2, count)),
                dma((n_width,)),
                dma((n_width,)),
                dma((n_rows,)),
                dma((n_rows,)),
                dma((n_rows,)),
                dma((n_rows,)),
                dma((2, reach, count)),
                dma((2, reach, count)),
                dma((1 + 2 * reach, count)),
                dma((1 + 2 * reach, count)),
            ],
            compiler_params=pltpu.CompilerParams(
                collective_id=0, has_side_effects=True, vmem_limit_bytes=24 * 1024 * 1024
            ),
        )(share, norm, one_query, other_query, one_key, other_key, one_value, other_value)
        final_query, final_key, final_value, col_query, col_key, col_value, norm_all = pl.pallas_call(
            store,
            out_shape=(
                jax.ShapeDtypeStruct((total, wide_query), jnp.bfloat16),
                jax.ShapeDtypeStruct((total, wide), jnp.bfloat16),
                jax.ShapeDtypeStruct((total, wide), jnp.bfloat16),
            )
            + tuple(jax.ShapeDtypeStruct(o.shape, o.dtype) for o in out_shape[count:]),
            in_specs=[vmem] * (count + 4),
            out_specs=[hbm] * 7,
            scratch_shapes=[dma((count + 4,))],
            compiler_params=pltpu.CompilerParams(vmem_limit_bytes=1024 * 1024),
        )(*gathered)
        serve_norm = norm_all[..., 0, :piece].astype(jnp.bfloat16).reshape(-1)
        return (
            final_query,
            final_key,
            final_value,
            col_query.reshape(-1),
            col_key.reshape(-1),
            col_value.reshape(-1),
            serve_norm,
        )

    wide_spec = P("rows", "width")
    in_specs = (wide_spec,) * 6 + (P("rows"), P(("rows", "width")), P(("rows", "width")))
    out_specs = (P(None, "width"),) * 3 + (P("width"),) * 3 + (P(),)
    return jax.shard_map(shards, mesh=mesh, in_specs=in_specs, out_specs=out_specs, check_vma=False)
```

```python
import jax
import jax.numpy as jnp
from jax import lax
from jax.experimental import pallas as pl
from jax.experimental.pallas import tpu as pltpu
from jax.sharding import PartitionSpec as P

MESH = pl.DeviceIdType.MESH
LANES = 128
WINDOW = 4
EARLY = 2


def kernel(
    n_rows,
    n_width,
    share_in,
    norm_train,
    norm_step,
    one_query,
    other_query,
    one_key,
    other_key,
    one_value,
    other_value,
    *refs,
):
    blocks = refs[: 2 + one_query.shape[1] // one_key.shape[1]]
    col_query, col_key, col_value, norm_all, first, second, share = refs[len(blocks) :][:7]
    part_early, part_late, in_sem, norm_send, norm_recv = refs[len(blocks) + 7 :][:5]
    slab_send, slab_recv, sum_send, sum_recv = refs[len(blocks) + 12 :][:4]
    ring_send, ring_recv, twin_send, twin_recv = refs[len(blocks) + 16 :]
    me = lax.axis_index("rows")
    lane = lax.axis_index("width")
    depth, wide = one_key.shape
    groups = [
        (one_key, other_key, blocks[0], col_key, 0),
        (one_value, other_value, blocks[1], col_value, 0),
    ] + [
        (one_query, other_query, blocks[2 + j], col_query, j * wide)
        for j in range(one_query.shape[1] // wide)
    ]
    tile = 64 if depth % 64 == 0 else 16
    half = depth // 2

    loads = []
    for g, (one, other, _, _, at) in enumerate(groups):
        a = pltpu.make_async_copy(one.at[:, pl.ds(at, wide)], first.at[g], in_sem.at[0, g])
        b = pltpu.make_async_copy(other.at[:, pl.ds(at, wide)], second.at[g], in_sem.at[1, g])
        loads.append((a, b))
        if g < WINDOW:
            a.start()
            b.start()

    norm_all[me, lane] = (norm_train[...] + norm_step[...]).reshape(1, -1)
    for at in range(0, depth, LANES):
        size = min(LANES, depth - at)
        line = share_in[pl.ds(at, size)].reshape(1, size)
        share[pl.ds(at, size), :] = jnp.broadcast_to(line, (LANES, size)).T

    barrier = pltpu.get_barrier_semaphore()
    for d in range(1, n_rows):
        pl.semaphore_signal(
            barrier, inc=1, device_id={"rows": lax.rem(me + d, n_rows)}, device_id_type=MESH
        )
    for d in range(1, n_width):
        pl.semaphore_signal(
            barrier, inc=1, device_id={"width": lax.rem(lane + d, n_width)}, device_id_type=MESH
        )
    pl.semaphore_wait(barrier, n_rows + n_width - 2)

    norm_copies = []
    for d in range(1, n_width):
        copy = pltpu.make_async_remote_copy(
            src_ref=norm_all.at[me, lane],
            dst_ref=norm_all.at[me, lane],
            send_sem=norm_send.at[d],
            recv_sem=norm_recv.at[d],
            device_id={"width": lax.rem(lane + d, n_width)},
            device_id_type=MESH,
        )
        copy.start()
        norm_copies.append(copy)

    def send_sums(part, kind):
        copies = []
        for d in range(1, n_rows):
            copy = pltpu.make_async_remote_copy(
                src_ref=part.at[me],
                dst_ref=part.at[me],
                send_sem=sum_send.at[kind, d],
                recv_sem=sum_recv.at[kind, d],
                device_id={"rows": lax.rem(me + d, n_rows)},
                device_id_type=MESH,
            )
            copy.start()
            copies.append(copy)
        return copies

    for g in range(len(groups)):
        for load in loads[g]:
            load.wait()
        for load in loads[g + WINDOW] if g + WINDOW < len(groups) else ():
            load.start()

        def mix(i, acc):
            rows = pl.ds(pl.multiple_of(i * tile, tile), tile)
            s = share[rows, :]
            s = jnp.concatenate([s] * (wide // LANES), axis=1)
            r = s * first[g, rows, :] + (1.0 - s) * second[g, rows, :]
            first[g, rows, :] = r
            return acc + jnp.sum((r * r).reshape(tile // 8, 8, wide), axis=0)

        acc = lax.fori_loop(0, depth // tile, mix, jnp.zeros((8, wide), jnp.float32))
        line = jnp.sum(acc, axis=0, keepdims=True)
        if g < EARLY:
            part_early[me, g] = line
        else:
            part_late[me, g - EARLY] = line
        if g == EARLY:
            early_copies = send_sums(part_early, 0)

    late_copies = send_sums(part_late, 1)

    for copy in norm_copies:
        copy.wait_recv()
    slab_copies = []
    for d in range(1, n_rows):
        copy = pltpu.make_async_remote_copy(
            src_ref=norm_all.at[me],
            dst_ref=norm_all.at[me],
            send_sem=slab_send.at[d],
            recv_sem=slab_recv.at[d],
            device_id={"rows": lax.rem(me + d, n_rows)},
            device_id_type=MESH,
        )
        copy.start()
        slab_copies.append(copy)

    core = lax.rem(me, 2)
    chip = me // 2
    chips = n_rows // 2
    reach = chips // 2

    def fold(c):
        return jnp.where(c < reach, c, 3 * reach - 1 - c)

    place = fold(chip)

    def device_at(step):
        return fold(lax.rem(place + step + chips, chips)) * 2 + core

    twin = me + 1 - 2 * core
    ahead = (device_at(1), device_at(-1))
    waits = []

    def region(g, owner, way, hop):
        if hop < reach:
            rows = pl.ds(pl.multiple_of(owner * depth, half), depth)
        else:
            rows = pl.ds(pl.multiple_of(owner * depth + way * half, half), half)
        return blocks[g].at[rows, :]

    def ring_copy(g, owner, way, hop):
        ref = region(g, owner, way, hop)
        copy = pltpu.make_async_remote_copy(
            src_ref=ref,
            dst_ref=ref,
            send_sem=ring_send.at[way, hop - 1, g],
            recv_sem=ring_recv.at[way, hop - 1, g],
            device_id={"rows": ahead[way]},
            device_id_type=MESH,
        )
        copy.start()
        return copy

    def twin_copy(g, owner, way, hop, slot):
        ref = region(g, owner, way, hop)
        copy = pltpu.make_async_remote_copy(
            src_ref=ref,
            dst_ref=ref,
            send_sem=twin_send.at[slot, g],
            recv_sem=twin_recv.at[slot, g],
            device_id={"rows": twin},
            device_id_type=MESH,
        )
        copy.start()
        waits.append(copy)

    flying = {}
    for g, (_, _, out, col, at) in enumerate(groups):
        if g in (0, EARLY):
            for copy in early_copies if g == 0 else late_copies:
                copy.wait_recv()
        part, line = (part_early, g) if g < EARLY else (part_late, g - EARLY)
        total = part[0, line]
        for p in range(1, n_rows):
            total = total + part[p, line]
        scale = jnp.sqrt(total)
        col[pl.ds(at, wide)] = scale.reshape(wide)
        inverse = 1.0 / scale

        def narrow(i, carry):
            rows = pl.ds(pl.multiple_of(i * tile, tile), tile)
            here = pl.ds(pl.multiple_of(me * depth + i * tile, tile), tile)
            out[here, :] = (first[g, rows, :] * inverse).astype(out.dtype)
            return carry

        lax.fori_loop(0, depth // tile, narrow, 0)
        for way in range(2):
            flying[way, 1, g] = ring_copy(g, me, way, 1)
        twin_copy(g, me, 0, 0, 0)

    for hop in range(1, reach + 1):
        for g in range(len(groups)):
            for way in range(2):
                copy = flying[way, hop, g]
                copy.wait_recv()
                owner = device_at(-hop if way == 0 else hop)
                if hop < reach:
                    flying[way, hop + 1, g] = ring_copy(g, owner, way, hop + 1)
                twin_copy(g, owner, way, hop, 1 + 2 * (hop - 1) + way)

    for copy in flying.values():
        copy.wait_send()
    for copy in waits:
        copy.wait()
    for copy in norm_copies + early_copies + late_copies:
        copy.wait_send()
    for copy in slab_copies:
        copy.wait()


def store(*refs):
    outs, sem = refs[-8:-1], refs[-1]
    blocks, small = refs[:-12], refs[-12:-8]
    wide = blocks[0].shape[1]
    pairs = [(blocks[0], outs[1]), (blocks[1], outs[2])] + list(zip(small, outs[3:]))
    for j, block in enumerate(blocks[2:]):
        pairs.append((block, outs[0].at[:, pl.ds(j * wide, wide)]))
    copies = [pltpu.make_async_copy(src, dst, sem.at[i]) for i, (src, dst) in enumerate(pairs)]
    for copy in copies:
        copy.start()
    for copy in copies:
        copy.wait()


def solution(mesh):
    n_rows, n_width = mesh.shape["rows"], mesh.shape["width"]

    def shards(
        one_query,
        other_query,
        one_key,
        other_key,
        one_value,
        other_value,
        mix_share,
        norm_train,
        norm_step,
    ):
        depth, wide = one_key.shape
        wide_query = one_query.shape[1]
        count = 2 + wide_query // wide
        piece = norm_train.shape[0]
        total = depth * n_rows
        reach = n_rows // 4
        hbm = pl.BlockSpec(memory_space=pltpu.HBM)
        vmem = pl.BlockSpec(memory_space=pltpu.VMEM)
        dma = pltpu.SemaphoreType.DMA
        out_shape = (pltpu.VMEM((total, wide), jnp.bfloat16),) * count + (
            pltpu.VMEM((wide_query,), jnp.float32),
            pltpu.VMEM((wide,), jnp.float32),
            pltpu.VMEM((wide,), jnp.float32),
            pltpu.VMEM((n_rows, n_width, 1, piece), jnp.float32),
        )
        gathered = pl.pallas_call(
            lambda *refs: kernel(n_rows, n_width, *refs),
            out_shape=out_shape,
            in_specs=[vmem] * 3 + [hbm] * 6,
            out_specs=[vmem] * (count + 4),
            scratch_shapes=[
                pltpu.VMEM((count, depth, wide), jnp.float32),
                pltpu.VMEM((count, depth, wide), jnp.float32),
                pltpu.VMEM((depth, LANES), jnp.float32),
                pltpu.VMEM((n_rows, EARLY, 1, wide), jnp.float32),
                pltpu.VMEM((n_rows, count - EARLY, 1, wide), jnp.float32),
                dma((2, count)),
                dma((n_width,)),
                dma((n_width,)),
                dma((n_rows,)),
                dma((n_rows,)),
                dma((2, n_rows)),
                dma((2, n_rows)),
                dma((2, reach, count)),
                dma((2, reach, count)),
                dma((1 + 2 * reach, count)),
                dma((1 + 2 * reach, count)),
            ],
            compiler_params=pltpu.CompilerParams(
                collective_id=0, has_side_effects=True, vmem_limit_bytes=24 * 1024 * 1024
            ),
        )(mix_share, norm_train, norm_step, one_query, other_query, one_key, other_key, one_value, other_value)
        final_query, final_key, final_value, col_query, col_key, col_value, norm_all = pl.pallas_call(
            store,
            out_shape=(
                jax.ShapeDtypeStruct((total, wide_query), jnp.bfloat16),
                jax.ShapeDtypeStruct((total, wide), jnp.bfloat16),
                jax.ShapeDtypeStruct((total, wide), jnp.bfloat16),
            )
            + tuple(jax.ShapeDtypeStruct(o.shape, o.dtype) for o in out_shape[count:]),
            in_specs=[vmem] * (count + 4),
            out_specs=[hbm] * 7,
            scratch_shapes=[dma((count + 4,))],
            compiler_params=pltpu.CompilerParams(vmem_limit_bytes=1024 * 1024),
        )(*gathered)
        serve_norm = norm_all[..., 0, :].astype(jnp.bfloat16).reshape(-1)
        return (
            final_query,
            final_key,
            final_value,
            col_query,
            col_key,
            col_value,
            serve_norm,
        )

    wide_spec = P("rows", "width")
    in_specs = (wide_spec,) * 6 + (P("rows"), P(("rows", "width")), P(("rows", "width")))
    out_specs = (P(None, "width"),) * 3 + (P("width"),) * 3 + (P(),)
    return jax.shard_map(shards, mesh=mesh, in_specs=in_specs, out_specs=out_specs, check_vma=False)
```
